8 devices in a mesh: rep: 2 (over y, z), dp: 4 (over x, core).
Axes of the slice: x: 2, y: 2, z: 1, core: 2. Of those that a mesh axis runs over, the one named last changes fastest.
Arguments:
- a: bfloat16 [8, 4, 4096, 1536], P(('rep', 'dp')), parts along dimension 0
- g: bfloat16 [8, 4, 4096, 3584], P(('rep', 'dp')), parts along dimension 0
Outputs:
- output: bfloat16 [8, 1536, 3584], P('rep'), parts along dimension 0
There are 2 independent parts. The reference program is written for one: setup_inputs(seed, part) draws one part's arguments, and reference() takes and returns one part's arrays. A program takes and returns all parts, laid end to end along the dimension named above; each array names one.
All inputs are finite; a program needn't handle non-finite values.
Results may differ from the reference program's by a relative error of at most 0.012.
Values are sent between devices in bfloat16 or wider.
A program may use at most 2 GiB of HBM per device.

```python
import jax
import jax.numpy as jnp
from jax import lax

DEVICES = 4
MATRICES = 4
TOKENS = 4096
D = 1536
FF = 3584


def setup_inputs(seed: int = 0, part: int = 0) -> dict:
    ka, kg, ks = (jax.random.fold_in(k, part) for k in jax.random.split(jax.random.key(seed), 3))
    size = 2.0 ** jax.random.uniform(ks, (DEVICES, MATRICES, 1, 1), jnp.float32, -1.0, 1.0)
    a = jax.random.normal(ka, (DEVICES, MATRICES, TOKENS, D), jnp.float32)
    g = size * jax.random.normal(kg, (DEVICES, MATRICES, TOKENS, FF), jnp.float32) * (DEVICES * TOKENS) ** -0.5
    return {"a": a.astype(jnp.bfloat16), "g": g.astype(jnp.bfloat16)}


def reference(a, g):
    def take(so_far, one):
        return so_far + jnp.einsum("ntd,ntf->ndf", *one, preferred_element_type=jnp.float32), None

    return lax.scan(take, jnp.zeros((MATRICES, D, FF), jnp.float32), (a, g))[0].astype(jnp.bfloat16)
```

```python
import jax
import jax.numpy as jnp
from jax import lax
from jax.experimental import pallas as pl
from jax.experimental.pallas import tpu as pltpu
from jax.sharding import PartitionSpec as P


WIDTHS = (
    (256, 256, 512, 1024, 1536),
    (2048, 1536),
    (2048, 1536),
    (1536, 1024, 512, 256, 256),
)
F_LAG = 3
VMEM = 67043328
ANY = pl.BlockSpec(memory_space=pl.ANY)


def _dot(a, g):
    return lax.dot_general(a, g, (((0,), (0,)), ((), ())), preferred_element_type=jnp.float32)


def _params(**kw):
    return dict(compiler_params=pltpu.CompilerParams(vmem_limit_bytes=VMEM), **kw)


def theirs(pos, a, g, dep, n, c0, c):
    k, d = a.shape[2:]
    half, ct = d // 2, min(c, 512)

    def body(pos, a_ref, g_ref, dep_ref, o_ref):
        o_ref[...] = _dot(a_ref[0, 0], g_ref[0, 0]).astype(o_ref.dtype)

    return pl.pallas_call(
        body,
        out_shape=jax.ShapeDtypeStruct((half, c), jnp.bfloat16),
        grid_spec=pltpu.PrefetchScalarGridSpec(
            num_scalar_prefetch=1,
            grid=(c // ct,),
            in_specs=[
                pl.BlockSpec((1, 1, k, half), lambda j, pos: (0, n, 0, 1 - pos[0])),
                pl.BlockSpec((1, 1, k, ct), lambda j, pos: (0, n, 0, c0 // ct + j)),
                ANY,
            ],
            out_specs=pl.BlockSpec((half, ct), lambda j, pos: (0, j)),
        ),
        **_params(cost_estimate=pl.CostEstimate(flops=2 * k * half * c, bytes_accessed=2 * k * (half + c), transcendentals=0)),
    )(pos, a, g, dep)


def mine(pos, a, g, r, dep, n, c0, c):
    k, d = a.shape[2:]
    half, quarter, ct = d // 2, d // 4, min(c, 512)

    def body(pos, a_ref, g_ref, r_ref, dep_ref, send_ref, own_ref):
        s = _dot(a_ref[0, 0], g_ref[0, 0]) + r_ref[...].astype(jnp.float32)
        first, second = s[:quarter], s[quarter:]
        on_first = pos[1] == 0
        own_ref[...] = jnp.where(on_first, first, second)
        send_ref[...] = jnp.where(on_first, second, first).astype(send_ref.dtype)

    return pl.pallas_call(
        body,
        out_shape=(
            jax.ShapeDtypeStruct((quarter, c), jnp.bfloat16),
            jax.ShapeDtypeStruct((quarter, c), jnp.float32),
        ),
        grid_spec=pltpu.PrefetchScalarGridSpec(
            num_scalar_prefetch=1,
            grid=(c // ct,),
            in_specs=[
                pl.BlockSpec((1, 1, k, half), lambda j, pos: (0, n, 0, pos[0])),
                pl.BlockSpec((1, 1, k, ct), lambda j, pos: (0, n, 0, c0 // ct + j)),
                pl.BlockSpec((half, ct), lambda j, pos: (0, j)),
                ANY,
            ],
            out_specs=(
                pl.BlockSpec((quarter, ct), lambda j, pos: (0, j)),
                pl.BlockSpec((quarter, ct), lambda j, pos: (0, j)),
            ),
        ),
        **_params(cost_estimate=pl.CostEstimate(flops=2 * k * half * c, bytes_accessed=2 * k * (half + c), transcendentals=0)),
    )(pos, a, g, r, dep)


def finish(pos, own, got, out, dep, shape, n, c0, c):
    quarter, ct = own.shape[0], min(c, 512)

    def body(pos, own_ref, got_ref, dep_ref, *rest):
        f_ref, o_ref = rest[-2:]
        f = (own_ref[...] + got_ref[...].astype(jnp.float32)).astype(f_ref.dtype)
        f_ref[...] = f
        o_ref[0] = f

    extra = () if out is None else (out,)
    return pl.pallas_call(
        body,
        out_shape=(jax.ShapeDtypeStruct((quarter, c), jnp.bfloat16), jax.ShapeDtypeStruct(shape, jnp.bfloat16)),
        grid_spec=pltpu.PrefetchScalarGridSpec(
            num_scalar_prefetch=1,
            grid=(c // ct,),
            in_specs=[pl.BlockSpec((quarter, ct), lambda j, pos: (0, j))] * 2 + [ANY] * (1 + len(extra)),
            out_specs=(
                pl.BlockSpec((quarter, ct), lambda j, pos: (0, j)),
                pl.BlockSpec((1, quarter, ct), lambda j, pos: (n, 2 * pos[0] + pos[1], c0 // ct + j)),
            ),
        ),
        input_output_aliases={4: 1} if extra else {},
        **_params(cost_estimate=pl.CostEstimate(flops=quarter * c * 600, bytes_accessed=quarter * c * 10, transcendentals=0)),
    )(pos, own, got, dep, *extra)


def place(pos, parts, out, dep, n, c0, c):
    quarter, ct = parts[0].shape[0], min(c, 512)
    tiles = c // ct

    def body(pos, z_ref, cf_ref, cz_ref, dep_ref, out_ref, o_ref):
        for s, ref in enumerate((z_ref, cf_ref, cz_ref)):
            @pl.when(pl.program_id(0) == s)
            def _():
                o_ref[0] = ref[...]

    def at(s):
        return lambda p, j, pos: (0, jnp.where(p == s, j, jnp.where(p < s, 0, tiles - 1)))

    def to(p, j, pos):
        core, x = jnp.where(p == 0, pos[0], 1 - pos[0]), jnp.where(p == 1, pos[1], 1 - pos[1])
        return n, 2 * core + x, c0 // ct + j

    return pl.pallas_call(
        body,
        out_shape=jax.ShapeDtypeStruct(out.shape, out.dtype),
        grid_spec=pltpu.PrefetchScalarGridSpec(
            num_scalar_prefetch=1,
            grid=(3, tiles),
            in_specs=[pl.BlockSpec((quarter, ct), at(s)) for s in range(3)] + [ANY] * 2,
            out_specs=pl.BlockSpec((1, quarter, ct), to),
        ),
        input_output_aliases={5: 0},
        **_params(cost_estimate=pl.CostEstimate(flops=quarter * c * 600, bytes_accessed=quarter * c * 12, transcendentals=0)),
    )(pos, *parts, dep, out)


def solution(mesh):
    over_x = [(0, 2), (2, 0), (1, 3), (3, 1)]
    over_core = [(0, 1), (1, 0), (2, 3), (3, 2)]

    def swap_x(t):
        return lax.ppermute(t, "dp", over_x)

    def swap_core(t):
        return lax.ppermute(t, "dp", over_core)

    def body(a, g):
        me = lax.axis_index("dp")
        pos = jnp.stack([lax.rem(me, 2), lax.div(me, 2)]).astype(jnp.int32)
        _, matrices, _, d = a.shape
        shape = (matrices, d, g.shape[3])
        chunks = []
        for n, widths in enumerate(WIDTHS):
            c0 = 0
            for c in widths:
                chunks.append((n, c0, c))
                c0 += c
        last = len(chunks)
        r, own, y, f, cf, z = {}, {}, {}, {}, {}, {}
        state = {"dep": pos, "out": None}

        def do_theirs(i):
            if i < last:
                t = theirs(pos, a, g, state["dep"], *chunks[i])
                state["dep"] = t
                r[i] = swap_core(t)

        def do_mine(i):
            send, own[i] = mine(pos, a, g, r[i], state["dep"], *chunks[i])
            state["dep"] = send
            y[i] = swap_x(send)

        def do_finish(i):
            f[i], state["out"] = finish(pos, own[i], y[i], state["out"], state["dep"], shape, *chunks[i])
            state["dep"] = f[i]
            z[i] = swap_x(f[i])
            cf[i] = swap_core(f[i])

        def do_place(i):
            cz = swap_core(z[i])
            state["out"] = place(pos, (z[i], cf[i], cz), state["out"], state["dep"], *chunks[i])

        do_theirs(0)
        for i in range(last):
            do_theirs(i + 1)
            do_mine(i)
            if i >= F_LAG:
                do_finish(i - F_LAG)
        for i in range(last - F_LAG, last):
            do_finish(i)
        for i in range(last):
            do_place(i)
        return state["out"]

    spec = P(("rep", "dp"))
    return jax.shard_map(body, mesh=mesh, in_specs=(spec, spec), out_specs=P("rep"), check_vma=False)
```

```python
import jax
import jax.numpy as jnp
from jax import lax
from jax.experimental import pallas as pl
from jax.experimental.pallas import tpu as pltpu
from jax.sharding import PartitionSpec as P


CT = 256
SENDS = 8
KEPT = 16
LAG = 8
PIECES = ((0, 0, 3584), (1, 0, 3584), (2, 0, 3584), (3, 0, 1536), (3, 1536, 1024), (3, 2560, 512), (3, 3072, 256), (3, 3328, 256))
VMEM = 67043328
ANY = pl.BlockSpec(memory_space=pl.ANY)
MESH = pl.DeviceIdType.MESH


def _dot(a, g):
    return lax.dot_general(a, g, (((0,), (0,)), ((), ())), preferred_element_type=jnp.float32)


def reduce_kernel(a, g, *refs):
    outs, scratch = refs[: len(PIECES)], refs[len(PIECES) :]
    abuf, gbuf, tsend, term, xsend, own, got, fbuf, a_sem, g_sem, ts_sem, tr_sem, xs_sem, xr_sem, f_sem = scratch
    _, matrices, _, d = a.shape
    half, quarter, per = d // 2, d // 4, g.shape[3] // CT
    tiles = matrices * per
    me = lax.axis_index("dp")
    core, x = lax.rem(me, 2), lax.div(me, 2)
    sibling, across = 2 * x + 1 - core, 2 * (1 - x) + core

    def load_a(n, side):
        first = pl.multiple_of(half * jnp.where(side == 0, 1 - core, core), half)
        s = lax.rem(n, 2)
        return pltpu.make_async_copy(a.at[0, n, :, pl.ds(first, half)], abuf.at[s, side], a_sem.at[s, side])

    def load_g(t):
        n, j = lax.div(t, per), lax.rem(t, per)
        s = lax.rem(t, 2)
        return pltpu.make_async_copy(g.at[0, n, :, pl.ds(pl.multiple_of(j * CT, CT), CT)], gbuf.at[s], g_sem.at[s])

    def send_term(t):
        s = lax.rem(t, 2)
        return pltpu.make_async_remote_copy(
            tsend.at[s], term.at[s], ts_sem.at[s], tr_sem.at[s], device_id={"dp": sibling}, device_id_type=MESH
        )

    def send_x(t):
        s = lax.rem(t, SENDS)
        return pltpu.make_async_remote_copy(
            xsend.at[s], got.at[t], xs_sem.at[s], xr_sem.at[t], device_id={"dp": across}, device_id_type=MESH
        )

    def store_f(u, out, c0):
        s = lax.rem(u, 2)
        at = pl.multiple_of(lax.rem(u, per) * CT - c0, CT)
        return pltpu.make_async_copy(fbuf.at[s], out.at[:, pl.ds(at, CT)], f_sem.at[s])

    def wait_f(u):
        s = lax.rem(u, 2)
        pltpu.make_async_copy(fbuf.at[s], outs[0].at[:, pl.ds(0, CT)], f_sem.at[s]).wait()

    def finish(u):
        send_x(u).wait_recv()

        @pl.when(u >= 2)
        def _():
            wait_f(u - 2)

        fbuf[lax.rem(u, 2)] = (own[lax.rem(u, KEPT)] + got[u].astype(jnp.float32)).astype(fbuf.dtype)
        for (n, c0, c), out in zip(PIECES, outs):
            lo = n * per + c0 // CT

            @pl.when((u >= lo) & (u < lo + c // CT))
            def _():
                store_f(u, out, c0).start()

    load_a(0, 0).start()
    load_g(0).start()
    barrier = pltpu.get_barrier_semaphore()
    for other in (sibling, across):
        pl.semaphore_signal(barrier, inc=1, device_id={"dp": other}, device_id_type=MESH)
    pl.semaphore_wait(barrier, 2)

    def step(t, _):
        n, j = lax.div(t, per), lax.rem(t, per)
        s, sa = lax.rem(t, 2), lax.rem(n, 2)

        @pl.when(j == 0)
        def _():
            load_a(n, 0).wait()

        load_g(t).wait()

        @pl.when(t == 0)
        def _():
            load_a(0, 1).start()

        @pl.when(t + 1 < tiles)
        def _():
            load_g(t + 1).start()

        @pl.when((j == 1) & (n + 1 < matrices))
        def _():
            load_a(n + 1, 0).start()
            load_a(n + 1, 1).start()

        @pl.when(t >= 2)
        def _():
            send_term(t - 2).wait_send()

        tsend[s] = _dot(abuf[sa, 0], gbuf[s]).astype(tsend.dtype)
        send_term(t).start()

        @pl.when(j == 0)
        def _():
            load_a(n, 1).wait()

        part = _dot(abuf[sa, 1], gbuf[s])
        send_term(t).wait_recv()
        total = part + term[s].astype(jnp.float32)
        on_first = x == 0
        own[lax.rem(t, KEPT)] = jnp.where(on_first, total[:quarter], total[quarter:])

        @pl.when(t >= SENDS)
        def _():
            send_x(t - SENDS).wait_send()

        xsend[lax.rem(t, SENDS)] = jnp.where(on_first, total[quarter:], total[:quarter]).astype(xsend.dtype)
        send_x(t).start()

        @pl.when(t >= LAG)
        def _():
            finish(t - LAG)

        return 0

    lax.fori_loop(0, tiles, step, 0)

    def rest(u, _):
        finish(u)
        return 0

    lax.fori_loop(tiles - LAG, tiles, rest, 0)

    def drain(t, _):
        send_x(t).wait_send()
        return 0

    lax.fori_loop(tiles - SENDS, tiles, drain, 0)
    for t in (tiles - 2, tiles - 1):
        send_term(t).wait_send()
        wait_f(t)


def reduce_to_quarters(a, g):
    _, matrices, k, d = a.shape
    half, quarter, tiles = d // 2, d // 4, matrices * (g.shape[3] // CT)
    flops = 2 * k * d * g.shape[3] * matrices
    return pl.pallas_call(
        reduce_kernel,
        out_shape=tuple(jax.ShapeDtypeStruct((quarter, c), jnp.bfloat16) for _, _, c in PIECES),
        in_specs=[ANY] * 2,
        out_specs=(ANY,) * len(PIECES),
        scratch_shapes=[
            pltpu.VMEM((2, 2, k, half), jnp.bfloat16),
            pltpu.VMEM((2, k, CT), jnp.bfloat16),
            pltpu.VMEM((2, half, CT), jnp.bfloat16),
            pltpu.VMEM((2, half, CT), jnp.bfloat16),
            pltpu.VMEM((SENDS, quarter, CT), jnp.bfloat16),
            pltpu.VMEM((KEPT, quarter, CT), jnp.float32),
            pltpu.VMEM((tiles, quarter, CT), jnp.bfloat16),
            pltpu.VMEM((2, quarter, CT), jnp.bfloat16),
            pltpu.SemaphoreType.DMA((2, 2)),
            pltpu.SemaphoreType.DMA((2,)),
            pltpu.SemaphoreType.DMA((2,)),
            pltpu.SemaphoreType.DMA((2,)),
            pltpu.SemaphoreType.DMA((SENDS,)),
            pltpu.SemaphoreType.DMA((tiles,)),
            pltpu.SemaphoreType.DMA((2,)),
        ],
        name="reduce",
        compiler_params=pltpu.CompilerParams(vmem_limit_bytes=VMEM, collective_id=0, has_side_effects=True),
        cost_estimate=pl.CostEstimate(flops=flops, bytes_accessed=2 * a.size + 2 * g.size, transcendentals=0),
    )(a, g)


def place(pos, mine, passed, out, dep, shape, n, c0, c, other_chip):
    quarter, ct = mine.shape[0], min(c, 512)
    tiles = c // ct

    def body(pos, mine_ref, passed_ref, dep_ref, *rest):
        o_ref = rest[-1]
        for s, ref in enumerate((mine_ref, passed_ref)):
            @pl.when(pl.program_id(0) == s)
            def _():
                o_ref[0] = ref[...]

    def to(p, j, pos):
        core = jnp.where(p == 0, pos[0], 1 - pos[0])
        return n, 2 * core + (1 - pos[1] if other_chip else pos[1]), c0 // ct + j

    extra = () if out is None else (out,)
    return pl.pallas_call(
        body,
        out_shape=jax.ShapeDtypeStruct(shape, jnp.bfloat16),
        grid_spec=pltpu.PrefetchScalarGridSpec(
            num_scalar_prefetch=1,
            grid=(2, tiles),
            in_specs=[
                pl.BlockSpec((quarter, ct), lambda p, j, pos: (0, jnp.where(p == 0, j, tiles - 1))),
                pl.BlockSpec((quarter, ct), lambda p, j, pos: (0, jnp.where(p == 1, j, 0))),
            ]
            + [ANY] * (1 + len(extra)),
            out_specs=pl.BlockSpec((1, quarter, ct), to),
        ),
        input_output_aliases={4: 0} if extra else {},
        compiler_params=pltpu.CompilerParams(vmem_limit_bytes=VMEM),
        cost_estimate=pl.CostEstimate(flops=quarter * c * 400, bytes_accessed=quarter * c * 8, transcendentals=0),
    )(pos, mine, passed, dep, *extra)


def solution(mesh):
    over_x = [(0, 2), (2, 0), (1, 3), (3, 1)]
    over_core = [(0, 1), (1, 0), (2, 3), (3, 2)]

    def swap(t, pairs):
        return lax.ppermute(t, "dp", pairs)

    def body(a, g):
        me = lax.axis_index("dp")
        pos = jnp.stack([lax.rem(me, 2), lax.div(me, 2)]).astype(jnp.int32)
        _, matrices, _, d = a.shape
        shape = (matrices, d, g.shape[3])
        f = reduce_to_quarters(a, g)
        z = [swap(t, over_x) for t in f]
        cf = [swap(t, over_core) for t in f]
        out = None
        for i, piece in enumerate(PIECES):
            out = place(pos, f[i], cf[i], out, pos, shape, *piece, False)
        for i, piece in enumerate(PIECES):
            cz = swap(z[i], over_core)
            out = place(pos, z[i], cz, out, pos, shape, *piece, True)
        return out

    spec = P(("rep", "dp"))
    return jax.shard_map(body, mesh=mesh, in_specs=(spec, spec), out_specs=P("rep"), check_vma=False)
```

```python
import jax
import jax.numpy as jnp
from jax import lax
from jax.experimental import pallas as pl
from jax.experimental.pallas import tpu as pltpu
from jax.sharding import PartitionSpec as P


CT = 512
SENDS = 4
KEPT = 6
LAG = 5
PIECES = ((0, 0, 3584), (1, 0, 3584), (2, 0, 3584), (3, 0, 1536), (3, 1536, 1024), (3, 2560, 512), (3, 3072, 512))
VMEM = 67043328
ANY = pl.BlockSpec(memory_space=pl.ANY)
MESH = pl.DeviceIdType.MESH


def _dot(a, g):
    return lax.dot_general(a, g, (((0,), (0,)), ((), ())), preferred_element_type=jnp.float32)


def reduce_kernel(a, g, *refs):
    outs, scratch = refs[: len(PIECES)], refs[len(PIECES) :]
    abuf, gbuf, tsend, term, pend, xsend, own, got, fbuf, a_sem, g_sem, ts_sem, tr_sem, xs_sem, xr_sem, f_sem = scratch
    _, matrices, _, d = a.shape
    half, quarter, per = d // 2, d // 4, g.shape[3] // CT
    tiles = matrices * per
    me = lax.axis_index("dp")
    core, x = lax.rem(me, 2), lax.div(me, 2)
    sibling, across = 2 * x + 1 - core, 2 * (1 - x) + core

    def load_a(n, side):
        first = pl.multiple_of(half * jnp.where(side == 0, 1 - core, core), half)
        s = lax.rem(n, 2)
        return pltpu.make_async_copy(a.at[0, n, :, pl.ds(first, half)], abuf.at[s, side], a_sem.at[s, side])

    def load_g(t):
        n, j = lax.div(t, per), lax.rem(t, per)
        s = lax.rem(t, 2)
        return pltpu.make_async_copy(g.at[0, n, :, pl.ds(pl.multiple_of(j * CT, CT), CT)], gbuf.at[s], g_sem.at[s])

    def send_term(t):
        s = lax.rem(t, 2)
        return pltpu.make_async_remote_copy(
            tsend.at[s], term.at[s], ts_sem.at[s], tr_sem.at[s], device_id={"dp": sibling}, device_id_type=MESH
        )

    def send_x(t):
        s = lax.rem(t, SENDS)
        return pltpu.make_async_remote_copy(
            xsend.at[s], got.at[t], xs_sem.at[s], xr_sem.at[t], device_id={"dp": across}, device_id_type=MESH
        )

    def store_f(u, out, c0):
        s = lax.rem(u, 2)
        at = pl.multiple_of(lax.rem(u, per) * CT - c0, CT)
        return pltpu.make_async_copy(fbuf.at[s], out.at[:, pl.ds(at, CT)], f_sem.at[s])

    def wait_f(u):
        s = lax.rem(u, 2)
        pltpu.make_async_copy(fbuf.at[s], outs[0].at[:, pl.ds(0, CT)], f_sem.at[s]).wait()

    def finish(u):
        send_x(u).wait_recv()

        @pl.when(u >= 2)
        def _():
            wait_f(u - 2)

        fbuf[lax.rem(u, 2)] = (own[lax.rem(u, KEPT)] + got[u].astype(jnp.float32)).astype(fbuf.dtype)
        for (n, c0, c), out in zip(PIECES, outs):
            lo = n * per + c0 // CT

            @pl.when((u >= lo) & (u < lo + c // CT))
            def _():
                store_f(u, out, c0).start()

    def own_sum(t):
        send_term(t).wait_recv()

        @pl.when(t >= SENDS)
        def _():
            send_x(t - SENDS).wait_send()

        rows = [pl.ds(pl.multiple_of(quarter * q, quarter), quarter) for q in (x, 1 - x)]
        s = lax.rem(t, 2)
        own[lax.rem(t, KEPT)] = pend[rows[0], :] + term[s, rows[0], :].astype(jnp.float32)
        xsend[lax.rem(t, SENDS)] = (pend[rows[1], :] + term[s, rows[1], :].astype(jnp.float32)).astype(xsend.dtype)
        send_x(t).start()

    load_a(0, 0).start()
    load_g(0).start()
    barrier = pltpu.get_barrier_semaphore()
    for other in (sibling, across):
        pl.semaphore_signal(barrier, inc=1, device_id={"dp": other}, device_id_type=MESH)
    pl.semaphore_wait(barrier, 2)

    def step(t, _):
        n, j = lax.div(t, per), lax.rem(t, per)
        s, sa = lax.rem(t, 2), lax.rem(n, 2)

        @pl.when(j == 0)
        def _():
            load_a(n, 0).wait()

        load_g(t).wait()

        @pl.when(t == 0)
        def _():
            load_a(0, 1).start()

        @pl.when(t + 1 < tiles)
        def _():
            load_g(t + 1).start()

        @pl.when((j == 1) & (n + 1 < matrices))
        def _():
            load_a(n + 1, 0).start()
            load_a(n + 1, 1).start()

        @pl.when(t >= 2)
        def _():
            send_term(t - 2).wait_send()

        tsend[s] = _dot(abuf[sa, 0], gbuf[s]).astype(tsend.dtype)

        @pl.when(t >= 2)
        def _():
            own_sum(t - 1)

        send_term(t).start()

        @pl.when(j == 0)
        def _():
            load_a(n, 1).wait()

        pend[...] = _dot(abuf[sa, 1], gbuf[s])

        @pl.when(t == 0)
        def _():
            own_sum(0)

        @pl.when(t >= LAG)
        def _():
            finish(t - LAG)

        return 0

    lax.fori_loop(0, tiles, step, 0)
    own_sum(tiles - 1)

    def rest(u, _):
        finish(u)
        return 0

    lax.fori_loop(tiles - LAG, tiles, rest, 0)

    def drain(t, _):
        send_x(t).wait_send()
        return 0

    lax.fori_loop(tiles - SENDS, tiles, drain, 0)
    for t in (tiles - 2, tiles - 1):
        send_term(t).wait_send()
        wait_f(t)


def reduce_to_quarters(a, g):
    _, matrices, k, d = a.shape
    half, quarter, tiles = d // 2, d // 4, matrices * (g.shape[3] // CT)
    flops = 2 * k * d * g.shape[3] * matrices
    return pl.pallas_call(
        reduce_kernel,
        out_shape=tuple(jax.ShapeDtypeStruct((quarter, c), jnp.bfloat16) for _, _, c in PIECES),
        in_specs=[ANY] * 2,
        out_specs=(ANY,) * len(PIECES),
        scratch_shapes=[
            pltpu.VMEM((2, 2, k, half), jnp.bfloat16),
            pltpu.VMEM((2, k, CT), jnp.bfloat16),
            pltpu.VMEM((2, half, CT), jnp.bfloat16),
            pltpu.VMEM((2, half, CT), jnp.bfloat16),
            pltpu.VMEM((half, CT), jnp.float32),
            pltpu.VMEM((SENDS, quarter, CT), jnp.bfloat16),
            pltpu.VMEM((KEPT, quarter, CT), jnp.float32),
            pltpu.VMEM((tiles, quarter, CT), jnp.bfloat16),
            pltpu.VMEM((2, quarter, CT), jnp.bfloat16),
            pltpu.SemaphoreType.DMA((2, 2)),
            pltpu.SemaphoreType.DMA((2,)),
            pltpu.SemaphoreType.DMA((2,)),
            pltpu.SemaphoreType.DMA((2,)),
            pltpu.SemaphoreType.DMA((SENDS,)),
            pltpu.SemaphoreType.DMA((tiles,)),
            pltpu.SemaphoreType.DMA((2,)),
        ],
        name="reduce",
        compiler_params=pltpu.CompilerParams(vmem_limit_bytes=VMEM, collective_id=0, has_side_effects=True),
        cost_estimate=pl.CostEstimate(flops=flops, bytes_accessed=2 * a.size + 2 * g.size, transcendentals=0),
    )(a, g)


def place(pos, mine, passed, out, dep, shape, n, c0, c, other_chip):
    quarter, ct = mine.shape[0], min(c, 512)
    tiles = c // ct

    def body(pos, mine_ref, passed_ref, dep_ref, *rest):
        o_ref = rest[-1]
        for s, ref in enumerate((mine_ref, passed_ref)):
            @pl.when(pl.program_id(0) == s)
            def _():
                o_ref[0] = ref[...]

    def to(p, j, pos):
        core = jnp.where(p == 0, pos[0], 1 - pos[0])
        return n, 2 * core + (1 - pos[1] if other_chip else pos[1]), c0 // ct + j

    extra = () if out is None else (out,)
    return pl.pallas_call(
        body,
        out_shape=jax.ShapeDtypeStruct(shape, jnp.bfloat16),
        grid_spec=pltpu.PrefetchScalarGridSpec(
            num_scalar_prefetch=1,
            grid=(2, tiles),
            in_specs=[
                pl.BlockSpec((quarter, ct), lambda p, j, pos: (0, jnp.where(p == 0, j, tiles - 1))),
                pl.BlockSpec((quarter, ct), lambda p, j, pos: (0, jnp.where(p == 1, j, 0))),
            ]
            + [ANY] * (1 + len(extra)),
            out_specs=pl.BlockSpec((1, quarter, ct), to),
        ),
        input_output_aliases={4: 0} if extra else {},
        compiler_params=pltpu.CompilerParams(vmem_limit_bytes=VMEM),
        cost_estimate=pl.CostEstimate(flops=quarter * c * 400, bytes_accessed=quarter * c * 8, transcendentals=0),
    )(pos, mine, passed, dep, *extra)


def solution(mesh):
    over_x = [(0, 2), (2, 0), (1, 3), (3, 1)]
    over_core = [(0, 1), (1, 0), (2, 3), (3, 2)]

    def swap(t, pairs):
        return lax.ppermute(t, "dp", pairs)

    def body(a, g):
        me = lax.axis_index("dp")
        pos = jnp.stack([lax.rem(me, 2), lax.div(me, 2)]).astype(jnp.int32)
        _, matrices, _, d = a.shape
        shape = (matrices, d, g.shape[3])
        f = reduce_to_quarters(a, g)
        z = [swap(t, over_x) for t in f]
        cf = [swap(t, over_core) for t in f]
        out = None
        for i, piece in enumerate(PIECES):
            out = place(pos, f[i], cf[i], out, pos, shape, *piece, False)
        for i, piece in enumerate(PIECES):
            cz = swap(z[i], over_core)
            out = place(pos, z[i], cz, out, pos, shape, *piece, True)
        return out

    spec = P(("rep", "dp"))
    return jax.shard_map(body, mesh=mesh, in_specs=(spec, spec), out_specs=P("rep"), check_vma=False)
```

```python
import jax
import jax.numpy as jnp
from jax import lax
from jax.experimental import pallas as pl
from jax.experimental.pallas import tpu as pltpu
from jax.sharding import PartitionSpec as P


CT = 512
SENDS = 4
KEPT = 6
LAG = 5
PIECES = ((0, 0, 3584), (1, 0, 3584), (2, 0, 3584), (3, 0, 1536), (3, 1536, 1024), (3, 2560, 512), (3, 3072, 512))
VMEM = 67043328
ANY = pl.BlockSpec(memory_space=pl.ANY)
MESH = pl.DeviceIdType.MESH


def _dot(a, g):
    return lax.dot_general(a, g, (((0,), (0,)), ((), ())), preferred_element_type=jnp.float32)


def reduce_kernel(a, g, *refs):
    outs, scratch = refs[: len(PIECES)], refs[len(PIECES) :]
    abuf, gbuf, tsend, term, pend, xsend, own, got, fbuf, a_sem, g_sem, ts_sem, tr_sem, xs_sem, xr_sem, f_sem = scratch
    _, matrices, _, d = a.shape
    half, quarter, per = d // 2, d // 4, g.shape[3] // CT
    tiles = matrices * per
    me = lax.axis_index("dp")
    core, x = lax.rem(me, 2), lax.div(me, 2)
    sibling, across = 2 * x + 1 - core, 2 * (1 - x) + core

    def load_a(n, part):
        owner = core if part % 2 else 1 - core
        first = pl.multiple_of(half * owner + quarter * (1 - x if part < 2 else x), quarter)
        s = lax.rem(n, 2)
        return pltpu.make_async_copy(a.at[0, n, :, pl.ds(first, quarter)], abuf.at[s, part], a_sem.at[s, part])

    def load_g(t):
        n, j = lax.div(t, per), lax.rem(t, per)
        s = lax.rem(t, 2)
        return pltpu.make_async_copy(g.at[0, n, :, pl.ds(pl.multiple_of(j * CT, CT), CT)], gbuf.at[s], g_sem.at[s])

    def send_term(t, q):
        s = lax.rem(t, 2)
        return pltpu.make_async_remote_copy(
            tsend.at[s, q], term.at[s, q], ts_sem.at[s, q], tr_sem.at[s, q], device_id={"dp": sibling}, device_id_type=MESH
        )

    def send_x(t):
        s = lax.rem(t, SENDS)
        return pltpu.make_async_remote_copy(
            xsend.at[s], got.at[t], xs_sem.at[s], xr_sem.at[t], device_id={"dp": across}, device_id_type=MESH
        )

    def store_f(u, out, c0):
        s = lax.rem(u, 2)
        at = pl.multiple_of(lax.rem(u, per) * CT - c0, CT)
        return pltpu.make_async_copy(fbuf.at[s], out.at[:, pl.ds(at, CT)], f_sem.at[s])

    def wait_f(u):
        s = lax.rem(u, 2)
        pltpu.make_async_copy(fbuf.at[s], outs[0].at[:, pl.ds(0, CT)], f_sem.at[s]).wait()

    def finish(u):
        send_x(u).wait_recv()

        @pl.when(u >= 2)
        def _():
            wait_f(u - 2)

        fbuf[lax.rem(u, 2)] = (own[lax.rem(u, KEPT)] + got[u].astype(jnp.float32)).astype(fbuf.dtype)
        for (n, c0, c), out in zip(PIECES, outs):
            lo = n * per + c0 // CT

            @pl.when((u >= lo) & (u < lo + c // CT))
            def _():
                store_f(u, out, c0).start()

    load_a(0, 0).start()
    load_g(0).start()
    barrier = pltpu.get_barrier_semaphore()
    for other in (sibling, across):
        pl.semaphore_signal(barrier, inc=1, device_id={"dp": other}, device_id_type=MESH)
    pl.semaphore_wait(barrier, 2)

    def step(t, _):
        n, j = lax.div(t, per), lax.rem(t, per)
        s, sa = lax.rem(t, 2), lax.rem(n, 2)

        def need_a(part):
            @pl.when(j == 0)
            def _():
                load_a(n, part).wait()

            if part < 3:
                @pl.when(t == 0)
                def _():
                    load_a(0, part + 1).start()

        load_g(t).wait()

        @pl.when((t > 0) & (t + 1 < tiles))
        def _():
            load_g(t + 1).start()

        @pl.when((j == 1) & (n + 1 < matrices))
        def _():
            for part in range(4):
                load_a(n + 1, part).start()

        for q in range(2):
            need_a(2 * q)

            @pl.when(t >= 2)
            def _():
                send_term(t - 2, q).wait_send()

            tsend[s, q] = _dot(abuf[sa, 2 * q], gbuf[s]).astype(tsend.dtype)
            send_term(t, q).start()
            need_a(2 * q + 1)
            pend[...] = _dot(abuf[sa, 2 * q + 1], gbuf[s])
            send_term(t, q).wait_recv()
            total = pend[...] + term[s, q].astype(jnp.float32)
            if q == 1:
                own[lax.rem(t, KEPT)] = total
                continue

            @pl.when(t >= SENDS)
            def _():
                send_x(t - SENDS).wait_send()

            xsend[lax.rem(t, SENDS)] = total.astype(xsend.dtype)
            send_x(t).start()

            @pl.when(t == 0)
            def _():
                load_g(1).start()

        @pl.when(t >= LAG)
        def _():
            finish(t - LAG)

        return 0

    lax.fori_loop(0, tiles, step, 0)

    def rest(u, _):
        finish(u)
        return 0

    lax.fori_loop(tiles - LAG, tiles, rest, 0)

    def drain(t, _):
        send_x(t).wait_send()
        return 0

    lax.fori_loop(tiles - SENDS, tiles, drain, 0)
    for t in (tiles - 2, tiles - 1):
        for q in range(2):
            send_term(t, q).wait_send()
        wait_f(t)


def reduce_to_quarters(a, g):
    _, matrices, k, d = a.shape
    quarter, tiles = d // 4, matrices * (g.shape[3] // CT)
    flops = 2 * k * d * g.shape[3] * matrices
    return pl.pallas_call(
        reduce_kernel,
        out_shape=tuple(jax.ShapeDtypeStruct((quarter, c), jnp.bfloat16) for _, _, c in PIECES),
        in_specs=[ANY] * 2,
        out_specs=(ANY,) * len(PIECES),
        scratch_shapes=[
            pltpu.VMEM((2, 4, k, quarter), jnp.bfloat16),
            pltpu.VMEM((2, k, CT), jnp.bfloat16),
            pltpu.VMEM((2, 2, quarter, CT), jnp.bfloat16),
            pltpu.VMEM((2, 2, quarter, CT), jnp.bfloat16),
            pltpu.VMEM((quarter, CT), jnp.float32),
            pltpu.VMEM((SENDS, quarter, CT), jnp.bfloat16),
            pltpu.VMEM((KEPT, quarter, CT), jnp.float32),
            pltpu.VMEM((tiles, quarter, CT), jnp.bfloat16),
            pltpu.VMEM((2, quarter, CT), jnp.bfloat16),
            pltpu.SemaphoreType.DMA((2, 4)),
            pltpu.SemaphoreType.DMA((2,)),
            pltpu.SemaphoreType.DMA((2, 2)),
            pltpu.SemaphoreType.DMA((2, 2)),
            pltpu.SemaphoreType.DMA((SENDS,)),
            pltpu.SemaphoreType.DMA((tiles,)),
            pltpu.SemaphoreType.DMA((2,)),
        ],
        name="reduce",
        compiler_params=pltpu.CompilerParams(vmem_limit_bytes=VMEM, collective_id=0, has_side_effects=True),
        cost_estimate=pl.CostEstimate(flops=flops, bytes_accessed=2 * a.size + 2 * g.size, transcendentals=0),
    )(a, g)


def place(pos, mine, passed, out, dep, shape, n, c0, c, other_chip):
    quarter, ct = mine.shape[0], min(c, 512)
    tiles = c // ct

    def body(pos, mine_ref, passed_ref, dep_ref, *rest):
        o_ref = rest[-1]
        for s, ref in enumerate((mine_ref, passed_ref)):
            @pl.when(pl.program_id(0) == s)
            def _():
                o_ref[0] = ref[...]

    def to(p, j, pos):
        core = jnp.where(p == 0, pos[0], 1 - pos[0])
        return n, 2 * core + (1 - pos[1] if other_chip else pos[1]), c0 // ct + j

    extra = () if out is None else (out,)
    return pl.pallas_call(
        body,
        out_shape=jax.ShapeDtypeStruct(shape, jnp.bfloat16),
        grid_spec=pltpu.PrefetchScalarGridSpec(
            num_scalar_prefetch=1,
            grid=(2, tiles),
            in_specs=[
                pl.BlockSpec((quarter, ct), lambda p, j, pos: (0, jnp.where(p == 0, j, tiles - 1))),
                pl.BlockSpec((quarter, ct), lambda p, j, pos: (0, jnp.where(p == 1, j, 0))),
            ]
            + [ANY] * (1 + len(extra)),
            out_specs=pl.BlockSpec((1, quarter, ct), to),
        ),
        input_output_aliases={4: 0} if extra else {},
        compiler_params=pltpu.CompilerParams(vmem_limit_bytes=VMEM),
        cost_estimate=pl.CostEstimate(flops=quarter * c * 400, bytes_accessed=quarter * c * 8, transcendentals=0),
    )(pos, mine, passed, dep, *extra)


def solution(mesh):
    over_x = [(0, 2), (2, 0), (1, 3), (3, 1)]
    over_core = [(0, 1), (1, 0), (2, 3), (3, 2)]

    def swap(t, pairs):
        return lax.ppermute(t, "dp", pairs)

    def body(a, g):
        me = lax.axis_index("dp")
        pos = jnp.stack([lax.rem(me, 2), lax.div(me, 2)]).astype(jnp.int32)
        _, matrices, _, d = a.shape
        shape = (matrices, d, g.shape[3])
        f = reduce_to_quarters(a, g)
        z = [swap(t, over_x) for t in f]
        cf = [swap(t, over_core) for t in f]
        out = None
        for i, piece in enumerate(PIECES):
            out = place(pos, f[i], cf[i], out, pos, shape, *piece, False)
        for i, piece in enumerate(PIECES):
            cz = swap(z[i], over_core)
            out = place(pos, z[i], cz, out, pos, shape, *piece, True)
        return out

    spec = P(("rep", "dp"))
    return jax.shard_map(body, mesh=mesh, in_specs=(spec, spec), out_specs=P("rep"), check_vma=False)
```

```python
import jax
import jax.numpy as jnp
from jax import lax
from jax.experimental import pallas as pl
from jax.experimental.pallas import tpu as pltpu
from jax.sharding import PartitionSpec as P


CT = 512
SENDS = 8
PIECES = ((0, 0, 512), (0, 512, 3072), (1, 0, 3584), (2, 0, 3584), (3, 0, 1536), (3, 1536, 1024), (3, 2560, 512), (3, 3072, 512))
VMEM = 67043328
ANY = pl.BlockSpec(memory_space=pl.ANY)
MESH = pl.DeviceIdType.MESH


def _dot(a, g):
    return lax.dot_general(a, g, (((0,), (0,)), ((), ())), preferred_element_type=jnp.float32)


def reduce_kernel(a, g, *refs):
    outs, z0, scratch = refs[: len(PIECES)], refs[len(PIECES)], refs[len(PIECES) + 1 :]
    abuf, gbuf, tsend, term, pend, xsend, got, fbuf, first_f = scratch[:9]
    a_sem, g_sem, ts_sem, tr_sem, xs_sem, xr_sem, f_sem, z_sem = scratch[9:]
    _, matrices, _, d = a.shape
    half, quarter, per = d // 2, d // 4, g.shape[3] // CT
    tiles = matrices * per
    steps = 2 * tiles
    me = lax.axis_index("dp")
    core, x = lax.rem(me, 2), lax.div(me, 2)
    sibling, across = 2 * x + 1 - core, 2 * (1 - x) + core
    halves = [pl.ds(h * (CT // 2), CT // 2) for h in range(2)]

    def load_a(n, part):
        owner = core if part % 2 else 1 - core
        first = pl.multiple_of(half * owner + quarter * (1 - x if part < 2 else x), quarter)
        s = lax.rem(n, 2)
        return pltpu.make_async_copy(a.at[0, n, :, pl.ds(first, quarter)], abuf.at[s, part], a_sem.at[s, part])

    def turn(i):
        k = i - per
        alone = (i < per) | (i >= steps - per)
        p = jnp.where(alone, jnp.where(i < per, 0, 1), 1 - lax.rem(k + 2 * per, 2))
        t = jnp.where(alone, jnp.where(i < per, i, i - tiles), jnp.where(p == 0, per + lax.div(k, 2), lax.div(k, 2)))
        return p, t

    def load_g(i):
        _, t = turn(i)
        n, j = lax.div(t, per), lax.rem(t, per)
        s = lax.rem(i, 2)
        return pltpu.make_async_copy(g.at[0, n, :, pl.ds(pl.multiple_of(j * CT, CT), CT)], gbuf.at[s], g_sem.at[s])

    def load_first_g(h):
        return pltpu.make_async_copy(g.at[0, 0, :, halves[h]], gbuf.at[0, :, halves[h]], g_sem.at[2 * h])

    def to(other, src, dst, send_sem, recv_sem):
        return pltpu.make_async_remote_copy(src, dst, send_sem, recv_sem, device_id={"dp": other}, device_id_type=MESH)

    def send_term(i):
        s = lax.rem(i, 2)
        return to(sibling, tsend.at[s], term.at[s], ts_sem.at[s], tr_sem.at[s])

    def send_first_term(h):
        return to(sibling, tsend.at[0, :, halves[h]], term.at[0, :, halves[h]], ts_sem.at[2 * h], tr_sem.at[2 * h])

    def send_x(t):
        s = lax.rem(t, SENDS)
        return to(across, xsend.at[s], got.at[t], xs_sem.at[s], xr_sem.at[t])

    def send_first_x(h):
        return to(across, xsend.at[0, :, halves[h]], got.at[0, :, halves[h]], xs_sem.at[SENDS * h], xr_sem.at[tiles * h])

    def send_z():
        return to(across, first_f, z0, z_sem.at[0], z_sem.at[1])

    def store_f(u, out, c0):
        s = lax.rem(u, 2)
        at = pl.multiple_of(lax.rem(u, per) * CT - c0, CT)
        return pltpu.make_async_copy(fbuf.at[s], out.at[:, pl.ds(at, CT)], f_sem.at[s])

    def wait_f(u):
        s = lax.rem(u, 2)
        pltpu.make_async_copy(fbuf.at[s], outs[0].at[:, pl.ds(0, CT)], f_sem.at[s]).wait()

    def finish(u, s):
        @pl.when(u == 0)
        def _():
            for h in range(2):
                send_first_x(h).wait_recv()

        @pl.when(u > 0)
        def _():
            send_x(u).wait_recv()

        @pl.when(u >= 2)
        def _():
            wait_f(u - 2)

        f = (pend[...] + term[s].astype(jnp.float32) + got[u].astype(jnp.float32)).astype(fbuf.dtype)
        fbuf[lax.rem(u, 2)] = f

        @pl.when(u == 0)
        def _():
            first_f[...] = f

        for (n, c0, c), out in zip(PIECES, outs):
            lo = n * per + c0 // CT

            @pl.when((u >= lo) & (u < lo + c // CT))
            def _():
                store_f(u, out, c0).start()

    load_a(0, 0).start()
    load_first_g(0).start()
    barrier = pltpu.get_barrier_semaphore()
    for other in (sibling, across):
        pl.semaphore_signal(barrier, inc=1, device_id={"dp": other}, device_id_type=MESH)
    pl.semaphore_wait(barrier, 2)

    for h in range(2):
        if h == 0:
            load_a(0, 0).wait()
        load_first_g(h).wait()
        if h == 0:
            load_a(0, 1).start()
            load_first_g(1).start()
        else:
            load_g(1).start()
        tsend[0, :, halves[h]] = _dot(abuf[0, 0], gbuf[0, :, halves[h]]).astype(tsend.dtype)
        send_first_term(h).start()
        if h == 0:
            load_a(0, 1).wait()
        pend[:, halves[h]] = _dot(abuf[0, 1], gbuf[0, :, halves[h]])
        send_first_term(h).wait_recv()
        xsend[0, :, halves[h]] = (pend[:, halves[h]] + term[0, :, halves[h]].astype(jnp.float32)).astype(xsend.dtype)
        send_first_x(h).start()

    def step(i, _):
        p, t = turn(i)
        n, j = lax.div(t, per), lax.rem(t, per)
        s, sa = lax.rem(i, 2), lax.rem(n, 2)

        for q in range(2):

            @pl.when((p == q) & (j == 0))
            def _():
                load_a(n, 2 * q).wait()
                load_a(n, 2 * q + 1).wait()

            @pl.when((p == q) & (j == 2) & (n + 1 < matrices))
            def _():
                load_a(n + 1, 2 * q).start()
                load_a(n + 1, 2 * q + 1).start()

        load_g(i).wait()

        @pl.when(i + 1 < steps)
        def _():
            load_g(i + 1).start()

        @pl.when(i == 1)
        def _():
            for part in (2, 3):
                load_a(0, part).start()

        @pl.when(i == 2)
        def _():
            for h in range(2):
                send_first_term(h).wait_send()

        @pl.when(i > 2)
        def _():
            send_term(i - 2).wait_send()

        tsend[s] = _dot(abuf[sa, 2 * p], gbuf[s]).astype(tsend.dtype)
        send_term(i).start()
        pend[...] = _dot(abuf[sa, 2 * p + 1], gbuf[s])
        send_term(i).wait_recv()

        @pl.when(p == 0)
        def _():
            @pl.when(t == SENDS)
            def _():
                for h in range(2):
                    send_first_x(h).wait_send()

            @pl.when(t > SENDS)
            def _():
                send_x(t - SENDS).wait_send()

            xsend[lax.rem(t, SENDS)] = (pend[...] + term[s].astype(jnp.float32)).astype(xsend.dtype)
            send_x(t).start()

            @pl.when(t == tiles - 1)
            def _():
                send_z().start()

        @pl.when(p == 1)
        def _():
            finish(t, s)

        return 0

    lax.fori_loop(1, steps, step, 0)

    def drain(t, _):
        send_x(t).wait_send()
        return 0

    lax.fori_loop(tiles - SENDS, tiles, drain, 0)
    for i in (steps - 2, steps - 1):
        send_term(i).wait_send()
    for u in (tiles - 2, tiles - 1):
        wait_f(u)
    send_z().wait()


def reduce_to_quarters(a, g):
    _, matrices, k, d = a.shape
    quarter, tiles = d // 4, matrices * (g.shape[3] // CT)
    flops = 2 * k * d * g.shape[3] * matrices
    return pl.pallas_call(
        reduce_kernel,
        out_shape=tuple(jax.ShapeDtypeStruct((quarter, c), jnp.bfloat16) for c in [c for _, _, c in PIECES] + [CT]),
        in_specs=[ANY] * 2,
        out_specs=(ANY,) * (len(PIECES) + 1),
        scratch_shapes=[
            pltpu.VMEM((2, 4, k, quarter), jnp.bfloat16),
            pltpu.VMEM((2, k, CT), jnp.bfloat16),
            pltpu.VMEM((2, quarter, CT), jnp.bfloat16),
            pltpu.VMEM((2, quarter, CT), jnp.bfloat16),
            pltpu.VMEM((quarter, CT), jnp.float32),
            pltpu.VMEM((SENDS, quarter, CT), jnp.bfloat16),
            pltpu.VMEM((tiles, quarter, CT), jnp.bfloat16),
            pltpu.VMEM((2, quarter, CT), jnp.bfloat16),
            pltpu.VMEM((quarter, CT), jnp.bfloat16),
            pltpu.SemaphoreType.DMA((2, 4)),
            pltpu.SemaphoreType.DMA((3,)),
            pltpu.SemaphoreType.DMA((3,)),
            pltpu.SemaphoreType.DMA((3,)),
            pltpu.SemaphoreType.DMA((SENDS + 1,)),
            pltpu.SemaphoreType.DMA((tiles + 1,)),
            pltpu.SemaphoreType.DMA((2,)),
            pltpu.SemaphoreType.DMA((2,)),
        ],
        name="reduce",
        compiler_params=pltpu.CompilerParams(vmem_limit_bytes=VMEM, collective_id=0, has_side_effects=True),
        cost_estimate=pl.CostEstimate(flops=flops, bytes_accessed=2 * a.size + 2 * g.size, transcendentals=0),
    )(a, g)


def place(pos, mine, passed, out, dep, shape, n, c0, c, other_chip):
    quarter, ct = mine.shape[0], min(c, 512)
    tiles = c // ct

    def body(pos, mine_ref, passed_ref, dep_ref, *rest):
        o_ref = rest[-1]
        for s, ref in enumerate((mine_ref, passed_ref)):
            @pl.when(pl.program_id(0) == s)
            def _():
                o_ref[0] = ref[...]

    def to(p, j, pos):
        core = jnp.where(p == 0, pos[0], 1 - pos[0])
        return n, 2 * core + (1 - pos[1] if other_chip else pos[1]), c0 // ct + j

    extra = () if out is None else (out,)
    return pl.pallas_call(
        body,
        out_shape=jax.ShapeDtypeStruct(shape, jnp.bfloat16),
        grid_spec=pltpu.PrefetchScalarGridSpec(
            num_scalar_prefetch=1,
            grid=(2, tiles),
            in_specs=[
                pl.BlockSpec((quarter, ct), lambda p, j, pos: (0, jnp.where(p == 0, j, tiles - 1))),
                pl.BlockSpec((quarter, ct), lambda p, j, pos: (0, jnp.where(p == 1, j, 0))),
            ]
            + [ANY] * (1 + len(extra)),
            out_specs=pl.BlockSpec((1, quarter, ct), to),
        ),
        input_output_aliases={4: 0} if extra else {},
        compiler_params=pltpu.CompilerParams(vmem_limit_bytes=VMEM),
        cost_estimate=pl.CostEstimate(flops=quarter * c * 400, bytes_accessed=quarter * c * 8, transcendentals=0),
    )(pos, mine, passed, dep, *extra)


def solution(mesh):
    over_x = [(0, 2), (2, 0), (1, 3), (3, 1)]
    over_core = [(0, 1), (1, 0), (2, 3), (3, 2)]

    def swap(t, pairs):
        return lax.ppermute(t, "dp", pairs)

    def body(a, g):
        me = lax.axis_index("dp")
        pos = jnp.stack([lax.rem(me, 2), lax.div(me, 2)]).astype(jnp.int32)
        _, matrices, _, d = a.shape
        shape = (matrices, d, g.shape[3])
        *f, z0 = reduce_to_quarters(a, g)
        z = [z0] + [swap(t, over_x) for i, t in enumerate(f) if i > 0]
        cf = [swap(t, over_core) for t in f]
        out = None
        for i, piece in enumerate(PIECES):
            out = place(pos, f[i], cf[i], out, pos, shape, *piece, False)
        for i, piece in enumerate(PIECES):
            cz = swap(z[i], over_core)
            out = place(pos, z[i], cz, out, pos, shape, *piece, True)
        return out

    spec = P(("rep", "dp"))
    return jax.shard_map(body, mesh=mesh, in_specs=(spec, spec), out_specs=P("rep"), check_vma=False)
```

```python
import jax
import jax.numpy as jnp
from jax import lax
from jax.experimental import pallas as pl
from jax.experimental.pallas import tpu as pltpu
from jax.sharding import PartitionSpec as P


CT = 512
SENDS = 8
PIECES = ((0, 0, 512), (0, 512, 3072), (1, 0, 3584), (2, 0, 3584), (3, 0, 1536), (3, 1536, 1024), (3, 2560, 512), (3, 3072, 256), (3, 3328, 256))
PARTS = 3
VMEM = 67043328
ANY = pl.BlockSpec(memory_space=pl.ANY)
MESH = pl.DeviceIdType.MESH


def _dot(a, g):
    return lax.dot_general(a, g, (((0,), (0,)), ((), ())), preferred_element_type=jnp.float32)


def reduce_kernel(a, g, *refs):
    outs, z0, scratch = refs[: len(PIECES)], refs[len(PIECES)], refs[len(PIECES) + 1 :]
    abuf, gbuf, tsend, term, pend, xsend, got, fbuf, first_f = scratch[:9]
    a_sem, g_sem, ts_sem, tr_sem, xs_sem, xr_sem, f_sem, z_sem = scratch[9:]
    _, matrices, _, d = a.shape
    half, quarter, per = d // 2, d // 4, g.shape[3] // CT
    tiles = matrices * per
    steps = 2 * tiles
    me = lax.axis_index("dp")
    core, x = lax.rem(me, 2), lax.div(me, 2)
    sibling, across = 2 * x + 1 - core, 2 * (1 - x) + core
    halves = [pl.ds(h * (CT // 2), CT // 2) for h in range(2)]

    def load_a(n, part):
        owner = core if part % 2 else 1 - core
        first = pl.multiple_of(half * owner + quarter * (1 - x if part < 2 else x), quarter)
        s = lax.rem(n, 2)
        return pltpu.make_async_copy(a.at[0, n, :, pl.ds(first, quarter)], abuf.at[s, part], a_sem.at[s, part])

    def turn(i):
        k = i - per
        alone = (i < per) | (i >= steps - per)
        p = jnp.where(alone, jnp.where(i < per, 0, 1), 1 - lax.rem(k + 2 * per, 2))
        t = jnp.where(alone, jnp.where(i < per, i, i - tiles), jnp.where(p == 0, per + lax.div(k, 2), lax.div(k, 2)))
        return p, t

    def load_g(i):
        _, t = turn(i)
        n, j = lax.div(t, per), lax.rem(t, per)
        s = lax.rem(i, 2)
        return pltpu.make_async_copy(g.at[0, n, :, pl.ds(pl.multiple_of(j * CT, CT), CT)], gbuf.at[s], g_sem.at[s])

    def load_first_g(h):
        return pltpu.make_async_copy(g.at[0, 0, :, halves[h]], gbuf.at[0, :, halves[h]], g_sem.at[2 * h])

    def to(other, src, dst, send_sem, recv_sem):
        return pltpu.make_async_remote_copy(src, dst, send_sem, recv_sem, device_id={"dp": other}, device_id_type=MESH)

    def send_term(i):
        s = lax.rem(i, 2)
        return to(sibling, tsend.at[s], term.at[s], ts_sem.at[s], tr_sem.at[s])

    def send_first_term(h):
        return to(sibling, tsend.at[0, :, halves[h]], term.at[0, :, halves[h]], ts_sem.at[2 * h], tr_sem.at[2 * h])

    def send_x(t):
        s = lax.rem(t, SENDS)
        return to(across, xsend.at[s], got.at[t], xs_sem.at[s], xr_sem.at[t])

    def send_first_x(h):
        return to(across, xsend.at[0, :, halves[h]], got.at[0, :, halves[h]], xs_sem.at[SENDS * h], xr_sem.at[tiles * h])

    def send_z():
        return to(across, first_f, z0, z_sem.at[0], z_sem.at[1])

    def store_f(u, out, c0):
        s = lax.rem(u, 2)
        if out.shape[1] < CT:
            return pltpu.make_async_copy(fbuf.at[s, :, pl.ds(c0 % CT, out.shape[1])], out, f_sem.at[s])
        at = pl.multiple_of(lax.rem(u, per) * CT - c0, CT)
        return pltpu.make_async_copy(fbuf.at[s], out.at[:, pl.ds(at, CT)], f_sem.at[s])

    def wait_f(u):
        s = lax.rem(u, 2)
        pltpu.make_async_copy(fbuf.at[s], outs[0].at[:, pl.ds(0, CT)], f_sem.at[s]).wait()

    def finish(u, s):
        @pl.when(u == 0)
        def _():
            for h in range(2):
                send_first_x(h).wait_recv()

        @pl.when(u > 0)
        def _():
            send_x(u).wait_recv()

        @pl.when(u >= 2)
        def _():
            wait_f(u - 2)

        f = (pend[...] + term[s].astype(jnp.float32) + got[u].astype(jnp.float32)).astype(fbuf.dtype)
        fbuf[lax.rem(u, 2)] = f

        @pl.when(u == 0)
        def _():
            first_f[...] = f

        for (n, c0, c), out in zip(PIECES, outs):
            lo = n * per + c0 // CT

            @pl.when((u >= lo) & (u < lo + pl.cdiv(c, CT)))
            def _():
                store_f(u, out, c0).start()

    load_a(0, 0).start()
    load_first_g(0).start()
    barrier = pltpu.get_barrier_semaphore()
    for other in (sibling, across):
        pl.semaphore_signal(barrier, inc=1, device_id={"dp": other}, device_id_type=MESH)
    pl.semaphore_wait(barrier, 2)

    for h in range(2):
        if h == 0:
            load_a(0, 0).wait()
        load_first_g(h).wait()
        if h == 0:
            load_a(0, 1).start()
            load_first_g(1).start()
        else:
            load_g(1).start()
        tsend[0, :, halves[h]] = _dot(abuf[0, 0], gbuf[0, :, halves[h]]).astype(tsend.dtype)
        send_first_term(h).start()
        if h == 0:
            load_a(0, 1).wait()
        pend[:, halves[h]] = _dot(abuf[0, 1], gbuf[0, :, halves[h]])
        send_first_term(h).wait_recv()
        xsend[0, :, halves[h]] = (pend[:, halves[h]] + term[0, :, halves[h]].astype(jnp.float32)).astype(xsend.dtype)
        send_first_x(h).start()

    def step(i, _):
        p, t = turn(i)
        n, j = lax.div(t, per), lax.rem(t, per)
        s, sa = lax.rem(i, 2), lax.rem(n, 2)

        for q in range(2):

            @pl.when((p == q) & (j == 0))
            def _():
                load_a(n, 2 * q).wait()
                load_a(n, 2 * q + 1).wait()

            @pl.when((p == q) & (j == 2) & (n + 1 < matrices))
            def _():
                load_a(n + 1, 2 * q).start()
                load_a(n + 1, 2 * q + 1).start()

        load_g(i).wait()

        @pl.when(i + 1 < steps)
        def _():
            load_g(i + 1).start()

        @pl.when(i == 1)
        def _():
            for part in (2, 3):
                load_a(0, part).start()

        @pl.when(i == 2)
        def _():
            for h in range(2):
                send_first_term(h).wait_send()

        @pl.when(i > 2)
        def _():
            send_term(i - 2).wait_send()

        tsend[s] = _dot(abuf[sa, 2 * p], gbuf[s]).astype(tsend.dtype)
        send_term(i).start()
        pend[...] = _dot(abuf[sa, 2 * p + 1], gbuf[s])
        send_term(i).wait_recv()

        @pl.when(p == 0)
        def _():
            @pl.when(t == SENDS)
            def _():
                for h in range(2):
                    send_first_x(h).wait_send()

            @pl.when(t > SENDS)
            def _():
                send_x(t - SENDS).wait_send()

            xsend[lax.rem(t, SENDS)] = (pend[...] + term[s].astype(jnp.float32)).astype(xsend.dtype)
            send_x(t).start()

            @pl.when(t == tiles - 1)
            def _():
                send_z().start()

        @pl.when(p == 1)
        def _():
            finish(t, s)

        return 0

    lax.fori_loop(1, steps, step, 0)

    def drain(t, _):
        send_x(t).wait_send()
        return 0

    lax.fori_loop(tiles - SENDS, tiles, drain, 0)
    for i in (steps - 2, steps - 1):
        send_term(i).wait_send()
    for u in (tiles - 2, tiles - 1):
        wait_f(u)
    send_z().wait()


def reduce_to_quarters(a, g):
    _, matrices, k, d = a.shape
    quarter, tiles = d // 4, matrices * (g.shape[3] // CT)
    flops = 2 * k * d * g.shape[3] * matrices
    return pl.pallas_call(
        reduce_kernel,
        out_shape=tuple(jax.ShapeDtypeStruct((quarter, c), jnp.bfloat16) for c in [c for _, _, c in PIECES] + [CT]),
        in_specs=[ANY] * 2,
        out_specs=(ANY,) * (len(PIECES) + 1),
        scratch_shapes=[
            pltpu.VMEM((2, 4, k, quarter), jnp.bfloat16),
            pltpu.VMEM((2, k, CT), jnp.bfloat16),
            pltpu.VMEM((2, quarter, CT), jnp.bfloat16),
            pltpu.VMEM((2, quarter, CT), jnp.bfloat16),
            pltpu.VMEM((quarter, CT), jnp.float32),
            pltpu.VMEM((SENDS, quarter, CT), jnp.bfloat16),
            pltpu.VMEM((tiles, quarter, CT), jnp.bfloat16),
            pltpu.VMEM((2, quarter, CT), jnp.bfloat16),
            pltpu.VMEM((quarter, CT), jnp.bfloat16),
            pltpu.SemaphoreType.DMA((2, 4)),
            pltpu.SemaphoreType.DMA((3,)),
            pltpu.SemaphoreType.DMA((3,)),
            pltpu.SemaphoreType.DMA((3,)),
            pltpu.SemaphoreType.DMA((SENDS + 1,)),
            pltpu.SemaphoreType.DMA((tiles + 1,)),
            pltpu.SemaphoreType.DMA((2,)),
            pltpu.SemaphoreType.DMA((2,)),
        ],
        name="reduce",
        compiler_params=pltpu.CompilerParams(vmem_limit_bytes=VMEM, collective_id=0, has_side_effects=True),
        cost_estimate=pl.CostEstimate(flops=flops, bytes_accessed=2 * a.size + 2 * g.size, transcendentals=0),
    )(a, g)


def place(mine, passed, out, shape, n, c0, c, other_chip):
    quarter = mine.shape[0]
    rows = quarter // PARTS

    def body(mine_ref, passed_ref, *rest):
        o_ref, buf, in_sem, out_sem = rest[-4:]
        me = lax.axis_index("dp")
        core, x = lax.rem(me, 2), lax.div(me, 2)
        copies = []
        for s, ref in enumerate((mine_ref, passed_ref)):
            first = quarter * (2 * (1 - core if s else core) + (1 - x if other_chip else x))
            for p in range(PARTS):
                part = buf.at[s, pl.ds(p * rows, rows)]
                to = o_ref.at[n, pl.ds(pl.multiple_of(first + p * rows, rows), rows), pl.ds(c0, c)]
                copies.append(
                    (
                        pltpu.make_async_copy(ref.at[pl.ds(p * rows, rows)], part, in_sem.at[s, p]),
                        pltpu.make_async_copy(part, to, out_sem.at[s, p]),
                    )
                )
        for load, _ in copies:
            load.start()
        for load, store in copies:
            load.wait()
            store.start()
        for _, store in copies:
            store.wait()

    extra = () if out is None else (out,)
    return pl.pallas_call(
        body,
        out_shape=jax.ShapeDtypeStruct(shape, jnp.bfloat16),
        in_specs=[ANY] * (2 + len(extra)),
        out_specs=ANY,
        scratch_shapes=[
            pltpu.VMEM((2, quarter, c), jnp.bfloat16),
            pltpu.SemaphoreType.DMA((2, PARTS)),
            pltpu.SemaphoreType.DMA((2, PARTS)),
        ],
        input_output_aliases={2: 0} if extra else {},
        compiler_params=pltpu.CompilerParams(vmem_limit_bytes=VMEM),
        cost_estimate=pl.CostEstimate(flops=quarter * c * 400, bytes_accessed=quarter * c * 8, transcendentals=0),
    )(mine, passed, *extra)


def solution(mesh):
    over_x = [(0, 2), (2, 0), (1, 3), (3, 1)]
    over_core = [(0, 1), (1, 0), (2, 3), (3, 2)]

    def swap(t, pairs):
        return lax.ppermute(t, "dp", pairs)

    def body(a, g):
        _, matrices, _, d = a.shape
        shape = (matrices, d, g.shape[3])
        *f, z0 = reduce_to_quarters(a, g)
        z = [z0] + [swap(t, over_x) for i, t in enumerate(f) if i > 0]
        cf = [swap(t, over_core) for t in f]
        out = None
        for i, piece in enumerate(PIECES):
            out = place(f[i], cf[i], out, shape, *piece, False)
        for i, piece in enumerate(PIECES):
            cz = swap(z[i], over_core)
            out = place(z[i], cz, out, shape, *piece, True)
        return out

    spec = P(("rep", "dp"))
    return jax.shard_map(body, mesh=mesh, in_specs=(spec, spec), out_specs=P("rep"), check_vma=False)
```
